32 devices in a mesh: cache: 4 (over x, core), expert: 8 (over z, y).
Axes of the slice: x: 2, y: 2, z: 4, core: 2. Of those that a mesh axis runs over, the one named last changes fastest.
Arguments:
- queries: bfloat16 [2, 32, 2048], P(None, 'expert'), may hold values from -16 to 16
- k_cache: bfloat16 [32, 4096, 256], P('expert', 'cache'), may hold values from -6 to 6
- v_cache: bfloat16 [32, 4096, 256], P('expert', 'cache'), may hold values from -6 to 6
- lengths: int32 [32], P('expert'), may hold values from 1 to 4094
- w_out: bfloat16 [2048, 2880], P('cache'), may hold values from -0.125 to 0.125
- norm_gain: float32 [2880], replicated, may hold values from 0.25 to 1.75
- w_gate: bfloat16 [8, 2880, 1440], P('cache', 'expert'), may hold values from -0.109375 to 0.109375
- w_up: bfloat16 [8, 2880, 1440], P('cache', 'expert'), may hold values from -0.109375 to 0.109375
- w_down: bfloat16 [8, 1440, 2880], P('cache', None, 'expert'), may hold values from -0.15625 to 0.15625
- expert_ids: int32 [2, 32, 4], P(None, 'expert'), may hold values from 0 to 7, all different within a row; in each aligned block of 4 rows (0 to 3, 4 to 7, ..., all dimensions but the last counted through in order) at most 2 rows name the same one
- gate_weights: float32 [2, 32, 4], P(None, 'expert'), may hold values from 0.1 to 1
Outputs:
- mixed: bfloat16 [2, 32, 2880], P(None, 'expert')
- gate_owner: bfloat16 [8, 2880, 1440], P('expert', None, 'cache')
- up_owner: bfloat16 [8, 2880, 1440], P('expert', None, 'cache')
- down_owner: bfloat16 [8, 1440, 2880], P('expert', 'cache')
The draws below stay inside these ranges and needn't reach their ends.
Inputs may be any that keep to these rules, and one draw needn't show every extreme that they name: `expert_ids`: in each step the 4 rows of one index of expert name one expert at most 2 times; a row names 4 different experts.
All inputs are finite; a program needn't handle non-finite values.
Results may differ from the reference program's by a relative error of at most 0.015.
Values may be sent and summed in bfloat16 or wider, within the bound.
A program may use at most 64 MiB of HBM per device.

```python
import math
import jax
import jax.numpy as jnp
import numpy as np
from jax import lax

D = 2880
FF = 1440
QH = 32
KVH = 4
HD = 64
TOP = 4
STEPS = 2
ROWS_DEV = 4
EXPERTS = 8
CAP = 2
ROWS = 32
LENGTH = 4096


def draw_queries(key, part):
    result = 2.5 * jax.random.truncated_normal(jax.random.fold_in(key, 1), -6.0, 6.0, (STEPS, ROWS, QH * HD), jnp.float32)
    return result.astype(jnp.bfloat16)


def draw_k_cache(key, part):
    result = jax.random.truncated_normal(jax.random.fold_in(key, 2), -6.0, 6.0, (ROWS, LENGTH, KVH * HD), jnp.float32)
    return result.astype(jnp.bfloat16)


def place_ends(values, rng, low, top_value):
    longest = values.shape.index(max(values.shape))
    spots = []
    for shift in (0, 1):
        where = [jax.random.randint(jax.random.fold_in(rng, axis), (), 0, length) for axis, length in enumerate(values.shape)]
        where[longest] = (where[longest] + shift) % values.shape[longest]
        spots.append(tuple(where))
    return values.at[spots[0]].set(low).at[spots[1]].set(top_value)


def steps_of(own_key, dims, cuts, smallest, top_value):
    gain, own = 1.0, jax.random.fold_in(own_key, 6)
    for dim, shards_of in cuts:
        draws = jnp.exp(jax.random.uniform(jax.random.fold_in(own, dim), (shards_of,), jnp.float32, smallest / len(cuts), top_value / len(cuts)))
        gain = gain * jnp.repeat(draws, dims[dim] // shards_of).reshape([-1 if axis == dim else 1 for axis in range(len(dims))])
    return gain


def deal_out(own_key, own, number, rows, count, top, bound, skew):
    sequence = jax.random.permutation(own_key, count)
    heavy_load, common = shares(count, rows * top, bound, skew, True), shares(count, rows * top, bound, skew, False)
    places = jnp.arange(count)

    def named(tallies, rotation):
        used = int((tallies > 0).sum())
        fixed = max(1, used // 4)
        moved = fixed + (places - fixed + rotation * (used - fixed)) % max(1, count - fixed)
        return jnp.zeros((count,), jnp.int32).at[sequence[jnp.where(places < fixed, places, moved)]].set(jnp.asarray(tallies, jnp.int32))

    tallies = jnp.where(number % 4 == 0, named(heavy_load, number // 4), named(common, number - number // 4 - 1))
    mixed = jax.random.permutation(jax.random.fold_in(own, 3), count)
    donor, taker = mixed[0:count // 2 * 2:2], mixed[1:count // 2 * 2:2]
    margin = jnp.minimum(tallies[donor] - 1, bound - tallies[taker]) // 2
    margin = jnp.where((donor == sequence[0]) | (taker == sequence[0]) | (tallies[taker] == 0), 0, jnp.maximum(margin, 0))
    moved = jax.random.randint(jax.random.fold_in(own, 4), (count // 2,), 0, 1 << 20) % (margin + 1)
    tallies = tallies.at[donor].add(-moved).at[taker].add(moved)
    labels = jnp.searchsorted(jnp.cumsum(tallies), jnp.arange(rows * top), side="right").astype(jnp.int32)
    listing = labels.reshape(top, rows).T
    listing = listing[jax.random.permutation(jax.random.fold_in(own, 1), rows)]
    rotation = jax.random.randint(jax.random.fold_in(own, 2), (rows, 1), 0, top)
    return jnp.take_along_axis(listing, (jnp.arange(top)[None, :] + rotation) % top, axis=1)


def shares(count, total, most, skew, full):
    weights = [(1 << 20) // math.isqrt(grade ** skew) + 1 for grade in range(1, count + 1)]
    largest = most if full else min(most, max(-(-total // count), total * weights[0] // sum(weights)))
    least = 1 if total - largest >= count - 1 else 0
    holding, spare = [largest] + [least] * (count - 1), total - largest - least * (count - 1)
    while spare > 0:
        free = [i for i in range(1, count) if holding[i] < largest] or [i for i in range(1, count) if holding[i] < most]
        whole, left = sum([weights[i] for i in free]), spare
        for i in free:
            addition = min(most - holding[i], max(1, left * weights[i] // whole), spare)
            holding[i] = holding[i] + addition
            spare = spare - addition
    return np.array(holding)


def gaussian(key, dims, deviation, reach, shards=(), kind=jnp.bfloat16):
    values = deviation * jax.random.normal(key, dims, jnp.float32)
    if shards:
        values = values * steps_of(key, dims, shards, -0.22, 0.18)
    return jnp.clip(values, -reach, reach).astype(kind)


def setup_inputs(seed: int = 0) -> dict:
    splits = jax.random.split(jax.random.key(seed), 12)
    queries = draw_queries(jax.random.fold_in(splits[11], 71), 0)
    k_cache = draw_k_cache(jax.random.fold_in(splits[11], 71), 0)
    v_cache = gaussian(splits[2], (ROWS, LENGTH, KVH * HD), 1.0, 6.0, ((0, 8), (1, 4)))
    lengths = place_ends(jax.random.randint(splits[3], (ROWS,), 1, LENGTH - 1), jax.random.fold_in(splits[3], 1), 1, (LENGTH - 1) - 1).astype(jnp.int32)
    w_out = gaussian(splits[4], (QH * HD, D), (QH * HD) ** -0.5, 0.125, ((0, 4),))
    norm_gain = jnp.clip(1.0 + 0.15 * jax.random.normal(splits[5], (D,), jnp.float32), 0.25, 1.75)
    w_gate = gaussian(splits[6], (EXPERTS, D, FF), D ** -0.5, 0.109375, ((0, 4), (1, 8)))
    w_up = gaussian(splits[7], (EXPERTS, D, FF), D ** -0.5, 0.109375, ((0, 4), (1, 8)))
    w_down = gaussian(splits[8], (EXPERTS, FF, D), FF ** -0.5, 0.15625, ((0, 4), (2, 8)))
    expert_ids_keys = jax.random.split(jax.random.fold_in(splits[9], 1), STEPS * ROWS // ROWS_DEV)
    expert_ids_turns = jax.random.permutation(jax.random.fold_in(splits[9], 3), STEPS * ROWS // ROWS_DEV)
    expert_ids = jax.vmap(lambda own, number: deal_out(jax.random.fold_in(splits[9], 2), own, number, ROWS_DEV, EXPERTS, TOP, CAP, 2))(expert_ids_keys, expert_ids_turns).reshape((STEPS, ROWS, TOP))
    gate_weights = jnp.clip(0.1 + 0.9 * jax.random.uniform(splits[10], (STEPS, ROWS, TOP), jnp.float32) ** steps_of(splits[10], (STEPS, ROWS, TOP), ((1, 8),), -0.2, 0.2), 0.1, 1.0)
    return {"queries": queries, "k_cache": k_cache, "v_cache": v_cache, "lengths": lengths, "w_out": w_out, "norm_gain": norm_gain, "w_gate": w_gate, "w_up": w_up, "w_down": w_down, "expert_ids": expert_ids, "gate_weights": gate_weights}


def attend_row(query_row, key_row, value_row, length_row):
    group_size = QH // KVH
    query_heads = query_row.astype(jnp.float32).reshape(STEPS, KVH, group_size, HD)
    key_heads = key_row.astype(jnp.float32).reshape(LENGTH, KVH, HD)
    value_heads = value_row.astype(jnp.float32).reshape(LENGTH, KVH, HD)
    scores = jnp.einsum('shgd,phd->shgp', query_heads, key_heads) / math.sqrt(HD)
    limit = length_row + jnp.arange(STEPS, dtype=jnp.int32) + 1
    visible = jnp.arange(LENGTH, dtype=jnp.int32)[None, :] < limit[:, None]
    visible = visible[:, None, None, :]
    highest = lax.optimization_barrier(jnp.max(jnp.where(visible, scores, -1e+30), axis=-1, keepdims=True))
    weights = jnp.where(visible, jnp.exp(scores - highest), 0.0)
    mass = lax.optimization_barrier(jnp.sum(weights, axis=-1))
    rounded = lax.optimization_barrier(weights.astype(jnp.bfloat16)).astype(jnp.float32)
    accum = jnp.einsum('shgp,phd->shgd', rounded, value_heads)
    return (accum / mass[..., None]).reshape(STEPS, QH * HD).astype(jnp.bfloat16)

def reference(queries, k_cache, v_cache, lengths, w_out, norm_gain, w_gate, w_up, w_down, expert_ids, gate_weights):
    outputs = lax.map(lambda inputs: attend_row(*inputs), (jnp.swapaxes(queries, 0, 1), k_cache, v_cache, lengths))
    heads_out = jnp.swapaxes(outputs, 0, 1).reshape(STEPS * ROWS, QH * HD)
    attention = jnp.dot(heads_out, w_out, preferred_element_type=jnp.float32)
    scale = lax.rsqrt(lax.optimization_barrier(jnp.mean(attention * attention, axis=-1, keepdims=True)) + 1e-05)
    normed = (attention * scale * norm_gain).astype(jnp.bfloat16)
    picked = (expert_ids[..., None] == jnp.arange(EXPERTS, dtype=jnp.int32)).astype(jnp.float32)
    coefficient = lax.optimization_barrier(jnp.sum(picked * gate_weights[..., None], axis=2)).reshape(STEPS * ROWS, EXPERTS)

    def one_expert(running, inputs):
        gate_matrix, up_matrix, down_matrix, column = inputs
        gate_value = jnp.dot(normed, gate_matrix, preferred_element_type=jnp.float32)
        up_value = jnp.dot(normed, up_matrix, preferred_element_type=jnp.float32)
        hidden = (jax.nn.silu(gate_value) * up_value).astype(jnp.bfloat16)
        expert_out = jnp.dot(hidden, down_matrix, preferred_element_type=jnp.float32).astype(jnp.bfloat16)
        expert_out = lax.optimization_barrier(expert_out).astype(jnp.float32)
        return (running + column[:, None] * expert_out, None)
    start = jnp.zeros((STEPS * ROWS, D), jnp.float32)
    combined, _ = lax.scan(one_expert, start, (w_gate, w_up, w_down, coefficient.T))
    mixed = (attention + combined).astype(jnp.bfloat16).reshape(STEPS, ROWS, D)
    return (mixed, w_gate, w_up, w_down)
```

```python
import functools
import math

import jax
import jax.numpy as jnp
from jax import lax
from jax.experimental import pallas as pl
from jax.experimental.pallas import tpu as pltpu
from jax.sharding import PartitionSpec as P

D = 2880
QH = 32
KVH = 4
HD = 64
TOP = 4

MESH = pl.DeviceIdType.MESH


def exchange_kernel(
    C, E, I, wg_hbm, wu_hbm, wd_hbm, go_hbm, uo_hbm, do_hbm,
    g_in, u_in, d_in, g_stage, u_stage, g_relay, u_relay, d_relay, g_own, u_own, d_recv, d_own,
    load_sem, send1, recv1, send2, recv2, local_sem, out_sem,
):
    c = lax.axis_index("cache")
    e = lax.axis_index("expert")
    rows = g_own.shape[1]
    width = g_own.shape[2]

    loads = [
        pltpu.make_async_copy(wd_hbm, d_in, load_sem.at[0]),
        pltpu.make_async_copy(wg_hbm, g_in, load_sem.at[1]),
        pltpu.make_async_copy(wu_hbm, u_in, load_sem.at[2]),
    ]
    for load in loads:
        load.start()

    barrier = pltpu.get_barrier_semaphore()
    for k in range(1, C):
        pl.semaphore_signal(barrier, inc=1, device_id=(lax.rem(c + k, C), e), device_id_type=MESH)
    for k in range(1, E):
        pl.semaphore_signal(barrier, inc=1, device_id=(c, lax.rem(e + k, E)), device_id_type=MESH)
    pl.semaphore_wait(barrier, C - 1 + E - 1)

    relays = (d_relay, g_relay, u_relay)
    finals = (d_recv, g_own, u_own)

    def own_part(w, target, i):
        if w == 0:
            return d_in.at[i, target]
        return (g_stage, u_stage)[w - 1].at[target, i]

    def first(w, k, i):
        target = lax.rem(c + k, C)
        return pltpu.make_async_remote_copy(
            src_ref=own_part(w, target, i),
            dst_ref=relays[w].at[c, i],
            send_sem=send1.at[w, target, i],
            recv_sem=recv1.at[w, c, i],
            device_id=(target, e),
            device_id_type=MESH,
        )

    def first_arrived(w, source, i):
        pltpu.make_async_remote_copy(
            src_ref=relays[w].at[source, i],
            dst_ref=relays[w].at[source, i],
            send_sem=send1.at[w, source, i],
            recv_sem=recv1.at[w, source, i],
            device_id=(source, e),
            device_id_type=MESH,
        ).wait_recv()

    def second_ref(w, k, i):
        source = lax.rem(c + C - k, C)
        owner = source * I + i
        part = own_part(w, c, i) if k == 0 else relays[w].at[source, i]
        return source, owner, part

    def second(w, k, i, action):
        source, owner, part = second_ref(w, k, i)

        @pl.when(owner != e)
        def _():
            copy = pltpu.make_async_remote_copy(
                src_ref=part,
                dst_ref=finals[w].at[e],
                send_sem=send2.at[w, source, i],
                recv_sem=recv2.at[w, e],
                device_id=(c, owner),
                device_id_type=MESH,
            )
            if action == "start":
                copy.start()
            else:
                copy.wait_send()

        @pl.when(owner == e)
        def _():
            copy = pltpu.make_async_copy(part, finals[w].at[e], local_sem.at[w])
            if action == "start":
                copy.start()
            else:
                copy.wait()

    order = [k for k in range(2, C)] + [1] if C > 2 else list(range(1, C))
    for w in range(3):
        loads[w].wait()
        for i in range(I):
            if w > 0:
                source = (g_in, u_in)[w - 1]
                stage = (g_stage, u_stage)[w - 1]
                for target in range(C):
                    stage[target, i] = source[i, :, target * width : (target + 1) * width]
            for k in order:
                first(w, k, i).start()
        for i in range(I):
            second(w, 0, i, "start")
    for w in range(3):
        for i in range(I):
            for k in [1] + order[:-1]:
                first_arrived(w, lax.rem(c + C - k, C), i)
                second(w, k, i, "start")
    outs = []
    for w in range(3):
        for k in range(C):
            for i in range(I):
                second(w, k, i, "wait")
        for k in range(1, E):
            source = lax.rem(e + k, E)
            pltpu.make_async_remote_copy(
                src_ref=finals[w].at[source],
                dst_ref=finals[w].at[source],
                send_sem=send2.at[w, 0, 0],
                recv_sem=recv2.at[w, source],
                device_id=(c, source),
                device_id_type=MESH,
            ).wait_recv()
        if w == 0:
            chunk = 8 * max(n for n in range(1, 16) if d_own.shape[0] % (8 * n) == 0)

            def assemble(t, carry):
                span = pl.ds(pl.multiple_of(t * chunk, chunk), chunk)
                d_own[span, :] = jnp.concatenate([d_recv[s, span, :] for s in range(E)], axis=-1)
                return carry

            lax.fori_loop(0, d_own.shape[0] // chunk, assemble, 0)
            done = pltpu.make_async_copy(d_own, do_hbm, out_sem.at[0])
        else:
            done = pltpu.make_async_copy(finals[w], (go_hbm, uo_hbm)[w - 1], out_sem.at[w])
        done.start()
        outs.append(done)
    for w in range(3):
        for i in range(I):
            for k in range(1, C):
                first(w, k, i).wait_send()
    for done in outs:
        done.wait()


def exchange(w_gate, w_up, w_down):
    C = lax.axis_size("cache")
    E = lax.axis_size("expert")
    I, rows, hidden_width = w_gate.shape
    width = hidden_width // C
    bf16 = jnp.bfloat16
    shape = jax.ShapeDtypeStruct
    any_spec = pl.BlockSpec(memory_space=pl.ANY)
    gate, up, down = pl.pallas_call(
        functools.partial(exchange_kernel, C, E, I),
        out_shape=(
            shape((E, rows, width), bf16),
            shape((E, rows, width), bf16),
            shape((width, E * rows), bf16),
        ),
        in_specs=[any_spec] * 3,
        out_specs=(any_spec,) * 3,
        scratch_shapes=[
            pltpu.VMEM((I, rows, hidden_width), bf16),
            pltpu.VMEM((I, rows, hidden_width), bf16),
            pltpu.VMEM((I, C, width, rows), bf16),
            pltpu.VMEM((C, I, rows, width), bf16),
            pltpu.VMEM((C, I, rows, width), bf16),
            pltpu.VMEM((C, I, rows, width), bf16),
            pltpu.VMEM((C, I, rows, width), bf16),
            pltpu.VMEM((C, I, width, rows), bf16),
            pltpu.VMEM((E, rows, width), bf16),
            pltpu.VMEM((E, rows, width), bf16),
            pltpu.VMEM((E, width, rows), bf16),
            pltpu.VMEM((width, E * rows), bf16),
            pltpu.SemaphoreType.DMA((3,)),
            pltpu.SemaphoreType.DMA((3, C, I)),
            pltpu.SemaphoreType.DMA((3, C, I)),
            pltpu.SemaphoreType.DMA((3, C, I)),
            pltpu.SemaphoreType.DMA((3, E)),
            pltpu.SemaphoreType.DMA((3,)),
            pltpu.SemaphoreType.DMA((3,)),
        ],
        compiler_params=pltpu.CompilerParams(
            collective_id=0, has_side_effects=True, vmem_limit_bytes=60 << 20
        ),
    )(w_gate, w_up, w_down.reshape(I, C, width, rows))
    return (
        gate.reshape(1, E * rows, width),
        up.reshape(1, E * rows, width),
        down.reshape(1, width, E * rows),
    )


def exchange_plain(w_gate, w_up, w_down):
    gate_owner, up_owner = (
        lax.all_to_all(
            lax.all_to_all(w, "cache", split_axis=2, concat_axis=0, tiled=True),
            "expert",
            split_axis=0,
            concat_axis=1,
            tiled=True,
        )
        for w in (w_gate, w_up)
    )
    down_owner = lax.all_to_all(
        lax.all_to_all(w_down, "cache", split_axis=1, concat_axis=0, tiled=True),
        "expert",
        split_axis=0,
        concat_axis=2,
        tiled=True,
    )
    return gate_owner, up_owner, down_owner


def joined(part, axis, combine):
    gathered = jax.tree.map(lambda a: lax.all_gather(a, axis), part)

    def take(source):
        return jax.tree.map(lambda a: lax.dynamic_index_in_dim(a, source, 0, False), gathered)

    return lax.fori_loop(
        1, lax.axis_size(axis), lambda source, state: combine(state, take(source)), take(0)
    )


def merge_partials(first, second):
    first_high, first_mass, first_accum = first
    second_high, second_mass, second_accum = second
    shared = jnp.maximum(first_high, second_high)
    first_factor = jnp.exp(first_high - shared)
    second_factor = jnp.exp(second_high - shared)
    head_width = first_accum.shape[-1] // first_high.shape[-1]
    accum = first_accum * jnp.repeat(first_factor, head_width, axis=-1) + second_accum * jnp.repeat(
        second_factor, head_width, axis=-1
    )
    return (shared, first_mass * first_factor + second_mass * second_factor, accum)


def shards(
    queries,
    k_cache,
    v_cache,
    lengths,
    w_out,
    norm_gain,
    w_gate,
    w_up,
    w_down,
    expert_ids,
    gate_weights,
):
    rows_local, hidden_local = w_gate.shape[1], w_gate.shape[2] // lax.axis_size("cache")
    fits = rows_local % 8 == 0 and hidden_local % 8 == 0 and w_gate.shape[0] * lax.axis_size("cache") == lax.axis_size("expert")
    gate_owner, up_owner, down_owner = (exchange if fits else exchange_plain)(w_gate, w_up, w_down)
    cache_count = lax.axis_size("cache")
    cache_place = lax.axis_index("cache")
    step_count = queries.shape[0]
    row_count = k_cache.shape[0]
    positions = k_cache.shape[1]
    group_size = QH // KVH
    query_heads = queries.reshape(step_count, row_count, KVH, group_size, HD)
    key_heads = k_cache.reshape(row_count, positions, KVH, HD)
    value_heads = v_cache.reshape(row_count, positions, KVH, HD)
    scores = jnp.einsum(
        "srhgd,rphd->srhgp", query_heads, key_heads, preferred_element_type=jnp.float32
    ) * (1.0 / math.sqrt(HD))
    position = cache_place * positions + jnp.arange(positions, dtype=jnp.int32)
    limit = lengths[None, :] + jnp.arange(step_count, dtype=jnp.int32)[:, None] + 1
    visible = (position[None, None, :] < limit[:, :, None])[:, :, None, None, :]
    highest = jnp.max(jnp.where(visible, scores, -1e30), axis=-1)
    weights = jnp.where(visible, jnp.exp(scores - highest[..., None]), 0.0)
    mass = jnp.sum(weights, axis=-1).reshape(step_count, row_count, QH)
    accum = jnp.einsum(
        "srhgp,rphd->srhgd",
        weights.astype(jnp.bfloat16),
        value_heads,
        preferred_element_type=jnp.float32,
    )
    accum = accum.reshape(step_count, row_count, QH * HD)
    highest = highest.reshape(step_count, row_count, QH)
    own_width = w_out.shape[0]
    all_high, all_mass, all_accum = joined((highest, mass, accum), "cache", merge_partials)
    heads_out = all_accum / jnp.repeat(all_mass, HD, axis=-1)
    own_out = lax.dynamic_slice_in_dim(heads_out, cache_place * own_width, own_width, 2)
    own_rows = own_out.astype(jnp.bfloat16).reshape(step_count * row_count, own_width)
    projected = jnp.dot(own_rows, w_out, preferred_element_type=jnp.float32)
    attention = lax.psum(projected, "cache")
    scale = lax.rsqrt(jnp.mean(attention * attention, axis=-1, keepdims=True) + 1e-05)
    normed = (attention * scale * norm_gain).astype(jnp.bfloat16).reshape(step_count, row_count, D)
    experts_total = w_gate.shape[0] * cache_count
    capacity = max(2, (row_count * TOP + experts_total - 1) // experts_total)
    expert_range = jnp.arange(experts_total, dtype=jnp.int32)
    onehot = (expert_ids[..., None] == expert_range).astype(jnp.float32)
    chosen = jnp.sum(onehot, axis=2)
    gate_map = jnp.sum(onehot * gate_weights[..., None], axis=2)
    earlier = jnp.tril(jnp.ones((row_count, row_count), jnp.float32), -1)
    ranks = jnp.einsum("rq,sqe->sre", earlier, chosen, precision=lax.Precision.HIGHEST)
    slot_table = (ranks[..., None] == jnp.arange(capacity, dtype=jnp.float32)).astype(
        jnp.float32
    ) * chosen[..., None]
    outgoing = jnp.einsum(
        "srec,srd->escd",
        slot_table.astype(jnp.bfloat16),
        normed,
        preferred_element_type=jnp.float32,
    )
    outgoing = outgoing.astype(jnp.bfloat16).reshape(experts_total, step_count * capacity, D)
    slots = lax.all_to_all(outgoing, "expert", split_axis=0, concat_axis=0, tiled=True)
    source_count = slots.shape[0]
    item_count = slots.shape[1]
    slot_rows = slots.reshape(source_count * item_count, D)
    gate_value = jnp.dot(slot_rows, gate_owner[0], preferred_element_type=jnp.float32)
    up_value = jnp.dot(slot_rows, up_owner[0], preferred_element_type=jnp.float32)
    hidden = (jax.nn.silu(gate_value) * up_value).astype(jnp.bfloat16)
    partial_out = jnp.dot(hidden, down_owner[0], preferred_element_type=jnp.float32).reshape(
        source_count, item_count, D
    )
    expert_out = lax.psum(partial_out, "cache").astype(jnp.bfloat16)
    returned = lax.all_to_all(expert_out, "expert", split_axis=0, concat_axis=0, tiled=True)
    back_width = returned.shape[-1]
    returned = returned.reshape(experts_total, step_count, capacity, back_width)
    combined = jnp.einsum(
        "srec,escd->srd",
        slot_table * gate_map[..., None],
        returned.astype(jnp.float32),
        precision=lax.Precision.HIGHEST,
    )
    attention_rows = attention.reshape(step_count, row_count, D)
    mixed = (attention_rows + combined).astype(jnp.bfloat16)
    return (mixed, gate_owner, up_owner, down_owner)


def solution(mesh):
    return jax.shard_map(
        shards,
        mesh=mesh,
        in_specs=(
            P(None, "expert", None),
            P("expert", "cache", None),
            P("expert", "cache", None),
            P("expert"),
            P("cache", None),
            P(),
            P("cache", "expert", None),
            P("cache", "expert", None),
            P("cache", None, "expert"),
            P(None, "expert", None),
            P(None, "expert", None),
        ),
        out_specs=(
            P(None, "expert", None),
            P("expert", None, "cache"),
            P("expert", None, "cache"),
            P("expert", "cache", None),
        ),
        check_vma=False,
    )
```

```python
import functools
import math

import jax
import jax.numpy as jnp
from jax import lax
from jax.experimental import pallas as pl
from jax.experimental.pallas import tpu as pltpu
from jax.sharding import PartitionSpec as P

D = 2880
QH = 32
KVH = 4
HD = 64
TOP = 4

MESH = pl.DeviceIdType.MESH


def exchange_kernel(
    C, E, I, wg_hbm, wu_hbm, wd_hbm, go_hbm, uo_hbm, do_hbm,
    g_in, u_in, d_in, g_stage, u_stage, g_relay, u_relay, d_relay, g_own, u_own, d_recv, d_own,
    load_sem, send1, recv1, send2, recv2, local_sem, out_sem,
):
    c = lax.axis_index("cache")
    e = lax.axis_index("expert")
    rows = g_own.shape[1]
    width = g_own.shape[2]

    loads = [
        pltpu.make_async_copy(wd_hbm, d_in, load_sem.at[0]),
        pltpu.make_async_copy(wg_hbm, g_in, load_sem.at[1]),
        pltpu.make_async_copy(wu_hbm, u_in, load_sem.at[2]),
    ]
    for load in loads:
        load.start()

    barrier = pltpu.get_barrier_semaphore()
    for k in range(1, C):
        pl.semaphore_signal(barrier, inc=1, device_id=(lax.rem(c + k, C), e), device_id_type=MESH)
    for k in range(1, E):
        pl.semaphore_signal(barrier, inc=1, device_id=(c, lax.rem(e + k, E)), device_id_type=MESH)
    pl.semaphore_wait(barrier, C - 1 + E - 1)

    relays = (d_relay, g_relay, u_relay)
    finals = (d_recv, g_own, u_own)

    def own_part(w, target, i):
        if w == 0:
            return d_in.at[i, target]
        return (g_stage, u_stage)[w - 1].at[target, i]

    def first(w, k, i):
        target = lax.rem(c + k, C)
        return pltpu.make_async_remote_copy(
            src_ref=own_part(w, target, i),
            dst_ref=relays[w].at[c, i],
            send_sem=send1.at[w, target, i],
            recv_sem=recv1.at[w, c, i],
            device_id=(target, e),
            device_id_type=MESH,
        )

    def first_arrived(w, source, i):
        pltpu.make_async_remote_copy(
            src_ref=relays[w].at[source, i],
            dst_ref=relays[w].at[source, i],
            send_sem=send1.at[w, source, i],
            recv_sem=recv1.at[w, source, i],
            device_id=(source, e),
            device_id_type=MESH,
        ).wait_recv()

    def second_ref(w, k, i):
        source = lax.rem(c + C - k, C)
        owner = source * I + i
        part = own_part(w, c, i) if k == 0 else relays[w].at[source, i]
        return source, owner, part

    def second(w, k, i, action):
        source, owner, part = second_ref(w, k, i)

        @pl.when(owner != e)
        def _():
            copy = pltpu.make_async_remote_copy(
                src_ref=part,
                dst_ref=finals[w].at[e],
                send_sem=send2.at[w, source, i],
                recv_sem=recv2.at[w, e],
                device_id=(c, owner),
                device_id_type=MESH,
            )
            if action == "start":
                copy.start()
            else:
                copy.wait_send()

        @pl.when(owner == e)
        def _():
            copy = pltpu.make_async_copy(part, finals[w].at[e], local_sem.at[w])
            if action == "start":
                copy.start()
            else:
                copy.wait()

    order = [k for k in range(2, C)] + [1] if C > 2 else list(range(1, C))
    for w in range(3):
        loads[w].wait()
        for i in range(I):
            if w > 0:
                source = (g_in, u_in)[w - 1]
                stage = (g_stage, u_stage)[w - 1]
                for target in range(C):
                    stage[target, i] = source[i, :, target * width : (target + 1) * width]
            for k in order:
                first(w, k, i).start()
        for i in range(I):
            second(w, 0, i, "start")
    for w in range(3):
        for i in range(I):
            for k in [1] + order[:-1]:
                first_arrived(w, lax.rem(c + C - k, C), i)
                second(w, k, i, "start")
    outs = []
    for w in range(3):
        for k in range(C):
            for i in range(I):
                second(w, k, i, "wait")
        for k in range(1, E):
            source = lax.rem(e + k, E)
            pltpu.make_async_remote_copy(
                src_ref=finals[w].at[source],
                dst_ref=finals[w].at[source],
                send_sem=send2.at[w, 0, 0],
                recv_sem=recv2.at[w, source],
                device_id=(c, source),
                device_id_type=MESH,
            ).wait_recv()
        if w == 0:
            chunk = 8 * max(n for n in range(1, 16) if d_own.shape[0] % (8 * n) == 0)

            def assemble(t, carry):
                span = pl.ds(pl.multiple_of(t * chunk, chunk), chunk)
                d_own[span, :] = jnp.concatenate([d_recv[s, span, :] for s in range(E)], axis=-1)
                return carry

            lax.fori_loop(0, d_own.shape[0] // chunk, assemble, 0)
            done = pltpu.make_async_copy(d_own, do_hbm, out_sem.at[0])
        else:
            done = pltpu.make_async_copy(finals[w], (go_hbm, uo_hbm)[w - 1], out_sem.at[w])
        done.start()
        outs.append(done)
    for w in range(3):
        for i in range(I):
            for k in range(1, C):
                first(w, k, i).wait_send()
    for done in outs:
        done.wait()


def exchange(w_gate, w_up, w_down):
    C = lax.axis_size("cache")
    E = lax.axis_size("expert")
    I, rows, hidden_width = w_gate.shape
    width = hidden_width // C
    bf16 = jnp.bfloat16
    shape = jax.ShapeDtypeStruct
    any_spec = pl.BlockSpec(memory_space=pl.ANY)
    gate, up, down = pl.pallas_call(
        functools.partial(exchange_kernel, C, E, I),
        out_shape=(
            shape((E, rows, width), bf16),
            shape((E, rows, width), bf16),
            shape((width, E * rows), bf16),
        ),
        in_specs=[any_spec] * 3,
        out_specs=(any_spec,) * 3,
        scratch_shapes=[
            pltpu.VMEM((I, rows, hidden_width), bf16),
            pltpu.VMEM((I, rows, hidden_width), bf16),
            pltpu.VMEM((I, C, width, rows), bf16),
            pltpu.VMEM((C, I, rows, width), bf16),
            pltpu.VMEM((C, I, rows, width), bf16),
            pltpu.VMEM((C, I, rows, width), bf16),
            pltpu.VMEM((C, I, rows, width), bf16),
            pltpu.VMEM((C, I, width, rows), bf16),
            pltpu.VMEM((E, rows, width), bf16),
            pltpu.VMEM((E, rows, width), bf16),
            pltpu.VMEM((E, width, rows), bf16),
            pltpu.VMEM((width, E * rows), bf16),
            pltpu.SemaphoreType.DMA((3,)),
            pltpu.SemaphoreType.DMA((3, C, I)),
            pltpu.SemaphoreType.DMA((3, C, I)),
            pltpu.SemaphoreType.DMA((3, C, I)),
            pltpu.SemaphoreType.DMA((3, E)),
            pltpu.SemaphoreType.DMA((3,)),
            pltpu.SemaphoreType.DMA((3,)),
        ],
        compiler_params=pltpu.CompilerParams(
            collective_id=0, has_side_effects=True, vmem_limit_bytes=60 << 20
        ),
    )(w_gate, w_up, w_down.reshape(I, C, width, rows))
    return (
        gate.reshape(1, E * rows, width),
        up.reshape(1, E * rows, width),
        down.reshape(1, width, E * rows),
    )


def exchange_plain(w_gate, w_up, w_down):
    gate_owner, up_owner = (
        lax.all_to_all(
            lax.all_to_all(w, "cache", split_axis=2, concat_axis=0, tiled=True),
            "expert",
            split_axis=0,
            concat_axis=1,
            tiled=True,
        )
        for w in (w_gate, w_up)
    )
    down_owner = lax.all_to_all(
        lax.all_to_all(w_down, "cache", split_axis=1, concat_axis=0, tiled=True),
        "expert",
        split_axis=0,
        concat_axis=2,
        tiled=True,
    )
    return gate_owner, up_owner, down_owner


def shards(
    queries,
    k_cache,
    v_cache,
    lengths,
    w_out,
    norm_gain,
    w_gate,
    w_up,
    w_down,
    expert_ids,
    gate_weights,
):
    rows_local, hidden_local = w_gate.shape[1], w_gate.shape[2] // lax.axis_size("cache")
    fits = rows_local % 8 == 0 and hidden_local % 8 == 0 and w_gate.shape[0] * lax.axis_size("cache") == lax.axis_size("expert")
    gate_owner, up_owner, down_owner = (exchange if fits else exchange_plain)(w_gate, w_up, w_down)
    cache_count = lax.axis_size("cache")
    cache_place = lax.axis_index("cache")
    step_count = queries.shape[0]
    row_count = k_cache.shape[0]
    positions = k_cache.shape[1]
    group_size = QH // KVH
    query_heads = queries.reshape(step_count, row_count, KVH, group_size, HD)
    key_heads = k_cache.reshape(row_count, positions, KVH, HD)
    value_heads = v_cache.reshape(row_count, positions, KVH, HD)
    scores = jnp.einsum(
        "srhgd,rphd->srhgp", query_heads, key_heads, preferred_element_type=jnp.float32
    ) * (1.0 / math.sqrt(HD))
    position = cache_place * positions + jnp.arange(positions, dtype=jnp.int32)
    limit = lengths[None, :] + jnp.arange(step_count, dtype=jnp.int32)[:, None] + 1
    visible = (position[None, None, :] < limit[:, :, None])[:, :, None, None, :]
    highest = jnp.max(jnp.where(visible, scores, -1e30), axis=-1)
    weights = jnp.where(visible, jnp.exp(scores - highest[..., None]), 0.0)
    mass = jnp.sum(weights, axis=-1).reshape(step_count, row_count, QH)
    accum = jnp.einsum(
        "srhgp,rphd->srhgd",
        weights.astype(jnp.bfloat16),
        value_heads,
        preferred_element_type=jnp.float32,
    )
    accum = accum.reshape(step_count, row_count, QH * HD)
    highest = highest.reshape(step_count, row_count, QH)
    own_width = w_out.shape[0]
    gathered = lax.all_gather(jnp.concatenate((accum, highest, mass), axis=-1), "cache")
    own_heads = own_width // HD
    all_high = gathered[..., QH * HD : QH * HD + QH]
    factor = jnp.exp(all_high - jnp.max(all_high, axis=0))
    all_mass = jnp.sum(gathered[..., QH * HD + QH :] * factor, axis=0)
    own_factor = lax.dynamic_slice_in_dim(factor / all_mass, cache_place * own_heads, own_heads, 3)
    own_accum = lax.dynamic_slice_in_dim(gathered, cache_place * own_width, own_width, 3)
    own_out = jnp.sum(own_accum * jnp.repeat(own_factor, HD, axis=-1), axis=0)
    own_rows = own_out.astype(jnp.bfloat16).reshape(step_count * row_count, own_width)
    projected = jnp.dot(own_rows, w_out, preferred_element_type=jnp.float32)
    attention = jnp.sum(lax.all_gather(projected, "cache"), axis=0)
    scale = lax.rsqrt(jnp.mean(attention * attention, axis=-1, keepdims=True) + 1e-05)
    normed = (attention * scale * norm_gain).astype(jnp.bfloat16).reshape(step_count, row_count, D)
    experts_total = w_gate.shape[0] * cache_count
    capacity = max(2, (row_count * TOP + experts_total - 1) // experts_total)
    expert_range = jnp.arange(experts_total, dtype=jnp.int32)
    onehot = (expert_ids[..., None] == expert_range).astype(jnp.float32)
    chosen = jnp.sum(onehot, axis=2)
    gate_map = jnp.sum(onehot * gate_weights[..., None], axis=2)
    earlier = jnp.tril(jnp.ones((row_count, row_count), jnp.float32), -1)
    ranks = jnp.einsum("rq,sqe->sre", earlier, chosen, precision=lax.Precision.HIGHEST)
    slot_table = (ranks[..., None] == jnp.arange(capacity, dtype=jnp.float32)).astype(
        jnp.float32
    ) * chosen[..., None]
    outgoing = jnp.einsum(
        "srec,srd->escd",
        slot_table.astype(jnp.bfloat16),
        normed,
        preferred_element_type=jnp.float32,
    )
    outgoing = outgoing.astype(jnp.bfloat16).reshape(experts_total, step_count * capacity, D)
    slots = lax.all_to_all(outgoing, "expert", split_axis=0, concat_axis=0, tiled=True)
    source_count = slots.shape[0]
    item_count = slots.shape[1]
    slot_rows = slots.reshape(source_count * item_count, D)
    gate_value = jnp.dot(slot_rows, gate_owner[0], preferred_element_type=jnp.float32)
    up_value = jnp.dot(slot_rows, up_owner[0], preferred_element_type=jnp.float32)
    hidden = (jax.nn.silu(gate_value) * up_value).astype(jnp.bfloat16)
    partial_out = jnp.dot(hidden, down_owner[0], preferred_element_type=jnp.float32).reshape(
        source_count, item_count, D
    )
    expert_out = partial_out.astype(jnp.bfloat16)
    returned = lax.all_to_all(expert_out, "expert", split_axis=0, concat_axis=0, tiled=True)
    back_width = returned.shape[-1]
    returned = returned.reshape(experts_total, step_count, capacity, back_width)
    combined = jnp.einsum(
        "srec,escd->srd",
        slot_table * gate_map[..., None],
        returned.astype(jnp.float32),
        precision=lax.Precision.HIGHEST,
    )
    attention_rows = attention.reshape(step_count, row_count, D)
    combined = jnp.sum(lax.all_gather(combined, "cache"), axis=0)
    mixed = (attention_rows + combined).astype(jnp.bfloat16)
    return (mixed, gate_owner, up_owner, down_owner)


def solution(mesh):
    return jax.shard_map(
        shards,
        mesh=mesh,
        in_specs=(
            P(None, "expert", None),
            P("expert", "cache", None),
            P("expert", "cache", None),
            P("expert"),
            P("cache", None),
            P(),
            P("cache", "expert", None),
            P("cache", "expert", None),
            P("cache", None, "expert"),
            P(None, "expert", None),
            P(None, "expert", None),
        ),
        out_specs=(
            P(None, "expert", None),
            P("expert", None, "cache"),
            P("expert", None, "cache"),
            P("expert", "cache", None),
        ),
        check_vma=False,
    )
```

```python
import functools
import math

import jax
import jax.numpy as jnp
from jax import lax
from jax.experimental import pallas as pl
from jax.experimental.pallas import tpu as pltpu
from jax.sharding import PartitionSpec as P

D = 2880
QH = 32
KVH = 4
HD = 64
TOP = 4

MESH = pl.DeviceIdType.MESH


def exchange_kernel(
    C, E, I, wg_hbm, wu_hbm, wd_hbm, go_hbm, uo_hbm, do_hbm,
    g_in, u_in, d_in, g_stage, u_stage, g_relay, u_relay, d_relay, g_own, u_own, d_recv, d_own,
    load_sem, send1, recv1, send2, recv2, local_sem, out_sem,
):
    c = lax.axis_index("cache")
    e = lax.axis_index("expert")
    rows = g_own.shape[1]
    width = g_own.shape[2]

    loads = [
        pltpu.make_async_copy(wd_hbm, d_in, load_sem.at[0]),
        pltpu.make_async_copy(wg_hbm, g_in, load_sem.at[1]),
        pltpu.make_async_copy(wu_hbm, u_in, load_sem.at[2]),
    ]
    for load in loads:
        load.start()

    barrier = pltpu.get_barrier_semaphore()
    for k in range(1, C):
        pl.semaphore_signal(barrier, inc=1, device_id=(lax.rem(c + k, C), e), device_id_type=MESH)
    for k in range(1, E):
        pl.semaphore_signal(barrier, inc=1, device_id=(c, lax.rem(e + k, E)), device_id_type=MESH)
    pl.semaphore_wait(barrier, C - 1 + E - 1)

    relays = (d_relay, g_relay, u_relay)
    finals = (d_recv, g_own, u_own)

    def own_part(w, target, i):
        if w == 0:
            return d_in.at[i, target]
        return (g_stage, u_stage)[w - 1].at[target, i]

    def first(w, k, i):
        target = lax.rem(c + k, C)
        return pltpu.make_async_remote_copy(
            src_ref=own_part(w, target, i),
            dst_ref=relays[w].at[c, i],
            send_sem=send1.at[w, target, i],
            recv_sem=recv1.at[w, c, i],
            device_id=(target, e),
            device_id_type=MESH,
        )

    def first_arrived(w, source, i):
        pltpu.make_async_remote_copy(
            src_ref=relays[w].at[source, i],
            dst_ref=relays[w].at[source, i],
            send_sem=send1.at[w, source, i],
            recv_sem=recv1.at[w, source, i],
            device_id=(source, e),
            device_id_type=MESH,
        ).wait_recv()

    def second_ref(w, k, i):
        source = lax.rem(c + C - k, C)
        owner = source * I + i
        part = own_part(w, c, i) if k == 0 else relays[w].at[source, i]
        return source, owner, part

    def second(w, k, i, action):
        source, owner, part = second_ref(w, k, i)

        @pl.when(owner != e)
        def _():
            copy = pltpu.make_async_remote_copy(
                src_ref=part,
                dst_ref=finals[w].at[e],
                send_sem=send2.at[w, source, i],
                recv_sem=recv2.at[w, e],
                device_id=(c, owner),
                device_id_type=MESH,
            )
            if action == "start":
                copy.start()
            else:
                copy.wait_send()

        @pl.when(owner == e)
        def _():
            copy = pltpu.make_async_copy(part, finals[w].at[e], local_sem.at[w])
            if action == "start":
                copy.start()
            else:
                copy.wait()

    order = [k for k in range(2, C)] + [1] if C > 2 else list(range(1, C))
    for w in range(3):
        loads[w].wait()
        for i in range(I):
            if w > 0:
                source = (g_in, u_in)[w - 1]
                stage = (g_stage, u_stage)[w - 1]
                for target in range(C):
                    stage[target, i] = source[i, :, target * width : (target + 1) * width]
            for k in order:
                first(w, k, i).start()
        for i in range(I):
            second(w, 0, i, "start")
    for w in range(3):
        for i in range(I):
            for k in [1] + order[:-1]:
                first_arrived(w, lax.rem(c + C - k, C), i)
                second(w, k, i, "start")
    outs = []
    for w in range(3):
        for k in range(C):
            for i in range(I):
                second(w, k, i, "wait")
        for k in range(1, E):
            source = lax.rem(e + k, E)
            pltpu.make_async_remote_copy(
                src_ref=finals[w].at[source],
                dst_ref=finals[w].at[source],
                send_sem=send2.at[w, 0, 0],
                recv_sem=recv2.at[w, source],
                device_id=(c, source),
                device_id_type=MESH,
            ).wait_recv()
        if w == 0:
            chunk = 8 * max(n for n in range(1, 16) if d_own.shape[0] % (8 * n) == 0)

            def assemble(t, carry):
                span = pl.ds(pl.multiple_of(t * chunk, chunk), chunk)
                d_own[span, :] = jnp.concatenate([d_recv[s, span, :] for s in range(E)], axis=-1)
                return carry

            lax.fori_loop(0, d_own.shape[0] // chunk, assemble, 0)
            done = pltpu.make_async_copy(d_own, do_hbm, out_sem.at[0])
        else:
            done = pltpu.make_async_copy(finals[w], (go_hbm, uo_hbm)[w - 1], out_sem.at[w])
        done.start()
        outs.append(done)
    for w in range(3):
        for i in range(I):
            for k in range(1, C):
                first(w, k, i).wait_send()
    for done in outs:
        done.wait()


def exchange(w_gate, w_up, w_down):
    C = lax.axis_size("cache")
    E = lax.axis_size("expert")
    I, rows, hidden_width = w_gate.shape
    width = hidden_width // C
    bf16 = jnp.bfloat16
    shape = jax.ShapeDtypeStruct
    any_spec = pl.BlockSpec(memory_space=pl.ANY)
    gate, up, down = pl.pallas_call(
        functools.partial(exchange_kernel, C, E, I),
        out_shape=(
            shape((E, rows, width), bf16),
            shape((E, rows, width), bf16),
            shape((width, E * rows), bf16),
        ),
        in_specs=[any_spec] * 3,
        out_specs=(any_spec,) * 3,
        scratch_shapes=[
            pltpu.VMEM((I, rows, hidden_width), bf16),
            pltpu.VMEM((I, rows, hidden_width), bf16),
            pltpu.VMEM((I, C, width, rows), bf16),
            pltpu.VMEM((C, I, rows, width), bf16),
            pltpu.VMEM((C, I, rows, width), bf16),
            pltpu.VMEM((C, I, rows, width), bf16),
            pltpu.VMEM((C, I, rows, width), bf16),
            pltpu.VMEM((C, I, width, rows), bf16),
            pltpu.VMEM((E, rows, width), bf16),
            pltpu.VMEM((E, rows, width), bf16),
            pltpu.VMEM((E, width, rows), bf16),
            pltpu.VMEM((width, E * rows), bf16),
            pltpu.SemaphoreType.DMA((3,)),
            pltpu.SemaphoreType.DMA((3, C, I)),
            pltpu.SemaphoreType.DMA((3, C, I)),
            pltpu.SemaphoreType.DMA((3, C, I)),
            pltpu.SemaphoreType.DMA((3, E)),
            pltpu.SemaphoreType.DMA((3,)),
            pltpu.SemaphoreType.DMA((3,)),
        ],
        compiler_params=pltpu.CompilerParams(
            collective_id=0, has_side_effects=True, vmem_limit_bytes=60 << 20
        ),
    )(w_gate, w_up, w_down.reshape(I, C, width, rows))
    return (
        gate.reshape(1, E * rows, width),
        up.reshape(1, E * rows, width),
        down.reshape(1, width, E * rows),
    )


def exchange_plain(w_gate, w_up, w_down):
    gate_owner, up_owner = (
        lax.all_to_all(
            lax.all_to_all(w, "cache", split_axis=2, concat_axis=0, tiled=True),
            "expert",
            split_axis=0,
            concat_axis=1,
            tiled=True,
        )
        for w in (w_gate, w_up)
    )
    down_owner = lax.all_to_all(
        lax.all_to_all(w_down, "cache", split_axis=1, concat_axis=0, tiled=True),
        "expert",
        split_axis=0,
        concat_axis=2,
        tiled=True,
    )
    return gate_owner, up_owner, down_owner


def shards(
    queries,
    k_cache,
    v_cache,
    lengths,
    w_out,
    norm_gain,
    w_gate,
    w_up,
    w_down,
    expert_ids,
    gate_weights,
):
    rows_local, hidden_local = w_gate.shape[1], w_gate.shape[2] // lax.axis_size("cache")
    fits = rows_local % 8 == 0 and hidden_local % 8 == 0 and w_gate.shape[0] * lax.axis_size("cache") == lax.axis_size("expert")
    gate_owner, up_owner, down_owner = (exchange if fits else exchange_plain)(w_gate, w_up, w_down)
    cache_count = lax.axis_size("cache")
    cache_place = lax.axis_index("cache")
    step_count = queries.shape[0]
    row_count = k_cache.shape[0]
    positions = k_cache.shape[1]
    group_size = QH // KVH
    heads = queries.reshape(step_count, row_count, KVH, group_size, HD).transpose(1, 2, 0, 3, 4)
    same = jnp.eye(KVH, dtype=jnp.float32)
    spread = heads[:, :, :, :, None, :] * same.astype(heads.dtype)[None, :, None, None, :, None]
    spread = spread.reshape(row_count, step_count * QH, KVH * HD)
    scores = jnp.einsum(
        "rnk,rpk->rnp", spread, k_cache, preferred_element_type=jnp.float32
    ) * (1.0 / math.sqrt(HD))
    position = cache_place * positions + jnp.arange(positions, dtype=jnp.int32)
    limit = lengths[:, None] + jnp.arange(step_count, dtype=jnp.int32)[None, :] + 1
    limit = jnp.broadcast_to(
        limit[:, None, :, None], (row_count, KVH, step_count, group_size)
    ).reshape(row_count, step_count * QH)
    visible = position[None, None, :] < limit[:, :, None]
    highest = jnp.max(jnp.where(visible, scores, -1e30), axis=-1)
    weights = jnp.where(visible, jnp.exp(scores - highest[..., None]), 0.0)
    mass = jnp.sum(weights, axis=-1)
    accum = jnp.einsum(
        "rnp,rpk->rnk",
        weights.astype(jnp.bfloat16),
        v_cache,
        preferred_element_type=jnp.float32,
    ).reshape(row_count, KVH, step_count, group_size, KVH, HD)
    accum = jnp.sum(accum * same[None, :, None, None, :, None], axis=4)

    def by_step(a):
        return jnp.moveaxis(a, 2, 0).reshape(step_count, row_count, -1)

    accum = by_step(accum)
    highest = by_step(highest.reshape(row_count, KVH, step_count, group_size))
    mass = by_step(mass.reshape(row_count, KVH, step_count, group_size))
    own_width = w_out.shape[0]
    gathered = lax.all_gather(jnp.concatenate((accum, highest, mass), axis=-1), "cache")
    own_heads = own_width // HD
    all_high = gathered[..., QH * HD : QH * HD + QH]
    factor = jnp.exp(all_high - jnp.max(all_high, axis=0))
    all_mass = jnp.sum(gathered[..., QH * HD + QH :] * factor, axis=0)
    own_factor = lax.dynamic_slice_in_dim(factor / all_mass, cache_place * own_heads, own_heads, 3)
    own_accum = lax.dynamic_slice_in_dim(gathered, cache_place * own_width, own_width, 3)
    own_out = jnp.sum(own_accum * jnp.repeat(own_factor, HD, axis=-1), axis=0)
    own_rows = own_out.astype(jnp.bfloat16).reshape(step_count * row_count, own_width)
    projected = jnp.dot(own_rows, w_out, preferred_element_type=jnp.float32)
    attention = jnp.sum(lax.all_gather(projected, "cache"), axis=0)
    scale = lax.rsqrt(jnp.mean(attention * attention, axis=-1, keepdims=True) + 1e-05)
    normed = (attention * scale * norm_gain).astype(jnp.bfloat16).reshape(step_count, row_count, D)
    experts_total = w_gate.shape[0] * cache_count
    capacity = max(2, (row_count * TOP + experts_total - 1) // experts_total)
    expert_range = jnp.arange(experts_total, dtype=jnp.int32)
    onehot = (expert_ids[..., None] == expert_range).astype(jnp.float32)
    chosen = jnp.sum(onehot, axis=2)
    gate_map = jnp.sum(onehot * gate_weights[..., None], axis=2)
    earlier = jnp.tril(jnp.ones((row_count, row_count), jnp.float32), -1)
    ranks = jnp.einsum("rq,sqe->sre", earlier, chosen, precision=lax.Precision.HIGHEST)
    slot_table = (ranks[..., None] == jnp.arange(capacity, dtype=jnp.float32)).astype(
        jnp.float32
    ) * chosen[..., None]
    outgoing = jnp.einsum(
        "srec,srd->escd",
        slot_table.astype(jnp.bfloat16),
        normed,
        preferred_element_type=jnp.float32,
    )
    outgoing = outgoing.astype(jnp.bfloat16).reshape(experts_total, step_count * capacity, D)
    slots = lax.all_to_all(outgoing, "expert", split_axis=0, concat_axis=0, tiled=True)
    source_count = slots.shape[0]
    item_count = slots.shape[1]
    slot_rows = slots.reshape(source_count * item_count, D)
    gate_value = jnp.dot(slot_rows, gate_owner[0], preferred_element_type=jnp.float32)
    up_value = jnp.dot(slot_rows, up_owner[0], preferred_element_type=jnp.float32)
    hidden = (jax.nn.silu(gate_value) * up_value).astype(jnp.bfloat16)
    partial_out = jnp.dot(hidden, down_owner[0], preferred_element_type=jnp.float32).reshape(
        source_count, item_count, D
    )
    expert_out = partial_out.astype(jnp.bfloat16)
    returned = lax.all_to_all(expert_out, "expert", split_axis=0, concat_axis=0, tiled=True)
    back_width = returned.shape[-1]
    returned = returned.reshape(experts_total, step_count, capacity, back_width)
    combined = jnp.einsum(
        "srec,escd->srd",
        slot_table * gate_map[..., None],
        returned.astype(jnp.float32),
        precision=lax.Precision.HIGHEST,
    )
    attention_rows = attention.reshape(step_count, row_count, D)
    combined = jnp.sum(lax.all_gather(combined, "cache"), axis=0)
    mixed = (attention_rows + combined).astype(jnp.bfloat16)
    return (mixed, gate_owner, up_owner, down_owner)


def solution(mesh):
    return jax.shard_map(
        shards,
        mesh=mesh,
        in_specs=(
            P(None, "expert", None),
            P("expert", "cache", None),
            P("expert", "cache", None),
            P("expert"),
            P("cache", None),
            P(),
            P("cache", "expert", None),
            P("cache", "expert", None),
            P("cache", None, "expert"),
            P(None, "expert", None),
            P(None, "expert", None),
        ),
        out_specs=(
            P(None, "expert", None),
            P("expert", None, "cache"),
            P("expert", None, "cache"),
            P("expert", "cache", None),
        ),
        check_vma=False,
    )
```
